256 devices in a mesh: tm: 16 (over x, z_lo, core), space: 16 (over z_hi, y).
Axes of the slice: x: 4, y: 4, z: 8 (z_hi: 4, z_lo: 2; z = z_hi * 2 + z_lo), core: 2. Of those that a mesh axis runs over, the one named last changes fastest.
Arguments:
- state_rhs: float32 [32, 32, 128, 128], P('tm', 'space'), may hold values from -5 to 9
- adjoint_rhs: float32 [32, 32, 128, 128], P('tm', 'space'), may hold values from -5 to 9
- reaction: float32 [32, 128, 128], P('space'), may hold values from 0.01 to 1
Outputs:
- state_out: float32 [32, 32, 128, 128], P('tm', 'space')
- adjoint_out: float32 [32, 32, 128, 128], P('tm', 'space')
The draws below stay inside these ranges and needn't reach their ends.
All inputs are finite; a program needn't handle non-finite values.
Results may differ from the reference program's by a relative error of at most 0.00021.
Values sent between devices are 32-bit elements; how exact they have to be, the bound alone decides.
No kernel may reach another device: no remote copies, remote signals or barrier semaphores. Data moves between devices by JAX's collectives and lax.ppermute only.
A program may use at most 64 MiB of HBM per device.

```python
import math
import jax
import jax.numpy as jnp
from jax import lax

STEPS = 32
SWEEPS = 12
NX = 128
NY = 128
NZ = 32


def smooth_source(key, salt):
    folded = jax.random.fold_in(key, salt)
    phase_key, noise_key = jax.random.split(folded, 2)
    phases = jax.random.uniform(phase_key, (4,), jnp.float32, 0.0, 2.0 * math.pi)
    moments = jnp.arange(STEPS, dtype=jnp.float32)
    depths = jnp.arange(NZ, dtype=jnp.float32)
    across = jnp.arange(NX, dtype=jnp.float32)
    along = jnp.arange(NY, dtype=jnp.float32)
    amplitude = 1.5
    contrast = 0.4
    noise = jnp.clip(jax.random.normal(noise_key, (STEPS, NZ, NX, NY), jnp.float32), -5.0, 5.0)
    profile = 1.0 + 0.3 * jnp.cos(2.0 * math.pi * moments / STEPS + phases[0])
    strength = jnp.exp(contrast * jnp.cos(2.0 * math.pi * depths / 16.0 + phases[1]))
    lateral = 1.0 + 0.3 * jnp.cos(2.0 * math.pi * across / NX + phases[2])[:, None] * jnp.cos(2.0 * math.pi * along / NY + phases[3])[None, :]
    smooth = amplitude * profile[:, None, None, None] * strength[None, :, None, None] * lateral[None, None, :, :]
    return smooth + noise


def draw_state_rhs(key, part):
    return smooth_source(key, 11)


def draw_adjoint_rhs(key, part):
    return smooth_source(key, 23)


def draw_reaction(key, part):
    spread = jax.random.uniform(jax.random.fold_in(key, 37), (NZ, NX, NY), jnp.float32, 0.0, 1.0)
    return 0.01 * jnp.exp(math.log(100.0) * spread)


def setup_inputs(seed: int = 0) -> dict:
    arg_keys = jax.random.split(jax.random.key(seed), 4)
    return {
        "state_rhs": draw_state_rhs(jax.random.fold_in(arg_keys[3], 71), 0),
        "adjoint_rhs": draw_adjoint_rhs(jax.random.fold_in(arg_keys[3], 71), 0),
        "reaction": draw_reaction(jax.random.fold_in(arg_keys[3], 71), 0),
    }


ALPHA = 0.1
MU = 1.0
BETA = 1.0


def coefficients(reaction, freqs):
    turn = 2.0 * math.pi * freqs.astype(jnp.float32) / STEPS
    rate = math.exp(math.log(ALPHA) / STEPS)
    lam_re = 1.0 - rate * jnp.cos(turn)
    lam_im = rate * jnp.sin(turn)
    shaped = (-1,) + (1,) * reaction.ndim
    d_re = lam_re.reshape(shaped) + MU * (6.0 + reaction)
    d_im = jnp.broadcast_to(lam_im.reshape(shaped), d_re.shape)
    den_re = d_re * d_re - d_im * d_im + BETA * BETA
    den_im = 2.0 * d_re * d_im
    magnitude = den_re * den_re + den_im * den_im
    inv_re = den_re / magnitude
    inv_im = -den_im / magnitude
    return (d_re * inv_re - d_im * inv_im, d_re * inv_im + d_im * inv_re, BETA * inv_re, BETA * inv_im)


def block_solve(coefficient, source):
    q_re, q_im, r_re, r_im = coefficient
    y_real = source[..., 0, :, :, :]
    y_imag = source[..., 1, :, :, :]
    p_real = source[..., 2, :, :, :]
    p_imag = source[..., 3, :, :, :]
    new_yre = q_re * y_real - q_im * y_imag + (r_re * p_real - r_im * p_imag)
    new_yim = q_re * y_imag + q_im * y_real + (r_re * p_imag + r_im * p_real)
    new_pre = q_re * p_real - q_im * p_imag - (r_re * y_real - r_im * y_imag)
    new_pim = q_re * p_imag + q_im * p_real - (r_re * y_imag + r_im * y_real)
    return jnp.stack((new_yre, new_yim, new_pre, new_pim), axis=-4)


def neighbour_sum(field):
    padded = jnp.pad(field, ((0, 0), (1, 1), (1, 1), (1, 1)))
    total = padded[:, 2:, 1:-1, 1:-1] + padded[:, :-2, 1:-1, 1:-1]
    total = total + padded[:, 1:-1, 2:, 1:-1] + padded[:, 1:-1, :-2, 1:-1]
    return total + padded[:, 1:-1, 1:-1, 2:] + padded[:, 1:-1, 1:-1, :-2]


def reference(state_rhs, adjoint_rhs, reaction):
    times = jnp.arange(STEPS, dtype=jnp.float32)
    growth = jnp.exp(math.log(ALPHA) * times / STEPS)[:, None, None, None]
    shrink = jnp.exp(-math.log(ALPHA) * times / STEPS)[:, None, None, None]
    state_hat = jnp.fft.fft(state_rhs * growth, axis=0)
    adjoint_hat = jnp.fft.fft(adjoint_rhs[::-1] * growth, axis=0)
    sources = jnp.stack((state_hat.real, state_hat.imag, adjoint_hat.real, adjoint_hat.imag), axis=1)

    def solve_one(inputs):
        freq_rhs, freq_index = inputs
        coefficient = tuple(member[0] for member in coefficients(reaction, freq_index[None]))
        field = block_solve(coefficient, freq_rhs)

        def sweep(sweep_index, current):
            return block_solve(coefficient, freq_rhs + MU * neighbour_sum(current))

        return lax.fori_loop(0, SWEEPS - 1, sweep, field)

    solved = lax.map(solve_one, (sources, jnp.arange(STEPS, dtype=jnp.int32)))
    state_back = jnp.fft.ifft(solved[:, 0] + 1j * solved[:, 1], axis=0).real * shrink
    adjoint_back = (jnp.fft.ifft(solved[:, 2] + 1j * solved[:, 3], axis=0).real * shrink)[::-1]
    return state_back, adjoint_back
```

```python
import math

import jax
import jax.numpy as jnp
from jax import lax
from jax.experimental import pallas as pl
from jax.experimental.pallas import tpu as pltpu
from jax.sharding import Mesh
from jax.sharding import PartitionSpec as P

STEPS = 32
SWEEPS = 12
ALPHA = 0.1
MU = 1.0
BETA = 1.0

TM = ("x", "zl", "core")
SPACE = ("zh", "y")

HALO = SWEEPS - 1
ROWS = 8
WINDOW = ROWS + 2 * HALO
FAR = HALO - ROWS


def place_of(index):
    ix, zl, core = index // 4, (index // 2) % 2, index % 2
    turn = (zl + ix) % 2
    return 4 * ix + 2 * turn + (core + turn) % 2


PLACE = [place_of(i) for i in range(16)]
HOLDER = [PLACE.index(p) for p in range(16)]


def my_place():
    ix, zl, core = lax.axis_index("x"), lax.axis_index("zl"), lax.axis_index("core")
    turn = (zl + ix) % 2
    return 4 * ix + 2 * turn + (core + turn) % 2


def my_freq():
    return lax.axis_index("zh") * 4 + lax.axis_index("y")


def add(a, b):
    return a[0] + b[0], a[1] + b[1]


def sub(a, b):
    return a[0] - b[0], a[1] - b[1]


def turned(a, k, n, sign):
    re, im = a
    if k == 0:
        return a
    if 4 * k == n:
        return (-im, re) if sign > 0 else (im, -re)
    if 8 * k == n:
        h = math.sqrt(0.5)
        return (h * (re - im), h * (im + re)) if sign > 0 else (h * (re + im), h * (im - re))
    if 8 * k == 3 * n:
        h = math.sqrt(0.5)
        return (-h * (re + im), h * (re - im)) if sign > 0 else (h * (im - re), -h * (re + im))
    c = math.cos(2.0 * math.pi * k / n)
    s = sign * math.sin(2.0 * math.pi * k / n)
    return c * re - s * im, c * im + s * re


def fourier(values, sign):
    n = len(values)
    if n == 1:
        return values
    even = fourier(values[0::2], sign)
    odd = fourier(values[1::2], sign)
    odd = [turned(odd[k], k, n, sign) for k in range(n // 2)]
    return [add(e, o) for e, o in zip(even, odd)] + [sub(e, o) for e, o in zip(even, odd)]


def growth(n):
    return math.exp(math.log(ALPHA) * n / STEPS)


def forward_kernel(times, reaction, out):
    first = pl.multiple_of(my_place() * ROWS, ROWS)
    for z in range(2):
        values = [
            (
                times[n // 2, 0, n % 2, z] * growth(n),
                times[(31 - n) // 2, 1, (31 - n) % 2, z] * growth(n),
            )
            for n in range(STEPS)
        ]
        hat = fourier(values, -1)
        here = reaction[z, pl.ds(first, ROWS), :]
        for k in range(16):
            out[k, 0, z] = hat[k][0]
            out[k, 1, z] = hat[k][1]
            out[k, 2, z] = hat[k + 16][0]
            out[k, 3, z] = hat[k + 16][1]
            out[k, 4, z] = here


def backward_kernel(solved, out):
    for z in range(2):
        values = [
            (solved[k % 16, 2 * (k // 16), z], solved[k % 16, 2 * (k // 16) + 1, z])
            for k in range(STEPS)
        ]
        back = fourier(values, 1)
        for n in range(STEPS):
            scale = 1.0 / (growth(n) * STEPS)
            out[n // 2, 0, n % 2, z] = back[n][0] * scale
            out[(31 - n) // 2, 1, (31 - n) % 2, z] = back[n][1] * scale


def sweep_kernel(left2, left1, own, right1, right2, out, src, coef, u0, u1):
    rate = math.exp(math.log(ALPHA) / STEPS)
    freq = my_freq()
    cos, sin = jnp.float32(1.0), jnp.float32(0.0)
    for k in range(1, 16):
        cos = jnp.where(freq == k, jnp.float32(math.cos(math.pi * k / 16)), cos)
        sin = jnp.where(freq == k, jnp.float32(math.sin(math.pi * k / 16)), sin)
    shift_re = (1.0 - rate * cos + 6.0 * MU, 1.0 + rate * cos + 6.0 * MU)
    shift_im = (BETA + rate * sin, BETA - rate * sin)
    start = my_place() * ROWS - HALO

    def prepare(ref, ref_row, row):
        inside = jnp.logical_and(start + row >= 0, start + row < 16 * ROWS)
        keep = jnp.where(inside, jnp.float32(1.0), jnp.float32(0.0))
        for j in range(4):
            at = slice(8 * j, 8 * j + 8)
            reaction = MU * ref[ref_row, 4, at, :]
            for f in range(2):
                d_re = reaction + shift_re[f]
                d_im = shift_im[f]
                scale = keep / (d_re * d_re + d_im * d_im)
                g_re = d_re * scale
                g_im = -d_im * scale
                re = ref[ref_row, 2 * f, at, :]
                im = ref[ref_row, 2 * f + 1, at, :]
                coef[row, 2 * f, at, :] = g_re
                coef[row, 2 * f + 1, at, :] = g_im
                src[row, 2 * f, at, :] = re
                src[row, 2 * f + 1, at, :] = im
                u0[row, 2 * f, at, :] = g_re * re - g_im * im
                u0[row, 2 * f + 1, at, :] = g_re * im + g_im * re

    def spread(ref, first, count):
        def step(i, carry):
            prepare(ref, i, first + i)
            return carry

        lax.fori_loop(0, count, step, 0)

    spread(left2, 0, FAR)
    spread(left1, FAR, ROWS)
    spread(own, HALO, ROWS)
    spread(right1, HALO + ROWS, ROWS)
    spread(right2, HALO + 2 * ROWS, FAR)

    lane = lax.broadcasted_iota(jnp.int32, (8, 128), 1)
    sublane = lax.broadcasted_iota(jnp.int32, (8, 128), 0)
    first_lane, last_lane = lane == 0, lane == 127
    first_sub, last_sub = sublane == 0, sublane == 7
    zero = jnp.zeros((8, 128), jnp.float32)

    def total(old, row, c):
        tiles = [old[row, c, 8 * j : 8 * j + 8, :] for j in range(4)]
        down = [pltpu.roll(t, 1, 0) for t in tiles]
        up = [pltpu.roll(t, 7, 0) for t in tiles]
        sums = []
        for j in range(4):
            at = slice(8 * j, 8 * j + 8)
            below = jnp.where(first_sub, down[j - 1] if j > 0 else zero, down[j])
            above = jnp.where(last_sub, up[j + 1] if j < 3 else zero, up[j])
            sides = jnp.where(first_lane, zero, pltpu.roll(tiles[j], 1, 1))
            sides = sides + jnp.where(last_lane, zero, pltpu.roll(tiles[j], 127, 1))
            outer = old[row - 1, c, at, :] + old[row + 1, c, at, :]
            sums.append((below + above) + outer + sides)
        return sums

    def sweep(old, m, store):
        def step(row, carry):
            for f in range(2):
                nb_re = total(old, row, 2 * f)
                nb_im = total(old, row, 2 * f + 1)
                for j in range(4):
                    at = slice(8 * j, 8 * j + 8)
                    s_re = src[row, 2 * f, at, :] + MU * nb_re[j]
                    s_im = src[row, 2 * f + 1, at, :] + MU * nb_im[j]
                    g_re = coef[row, 2 * f, at, :]
                    g_im = coef[row, 2 * f + 1, at, :]
                    store(row, 2 * f, at, g_re * s_re - g_im * s_im)
                    store(row, 2 * f + 1, at, g_re * s_im + g_im * s_re)
            return carry

        lax.fori_loop(m, WINDOW - m, step, 0)

    def into(ref, offset):
        def store(row, c, at, value):
            ref[row - offset, c, at, :] = value

        return store

    def two(i, carry):
        sweep(u0, 2 * i + 1, into(u1, 0))
        sweep(u1, 2 * i + 2, into(u0, 0))
        return carry

    lax.fori_loop(0, (SWEEPS - 2) // 2, two, 0)
    sweep(u0, SWEEPS - 1, into(out, HALO))


def f32(*shape):
    return jax.ShapeDtypeStruct(shape, jnp.float32)


def body(state_rhs, adjoint_rhs, reaction):
    both = jnp.stack((state_rhs, adjoint_rhs)).reshape(2, 2, 2, 16, ROWS, 128)
    both = jnp.stack([both[:, :, :, p] for p in PLACE])
    times = lax.all_to_all(both, TM, 0, 0, tiled=True)
    spread = pl.pallas_call(forward_kernel, out_shape=f32(16, 5, 2, ROWS, 128), name="forward")(
        times, reaction
    )
    got = lax.all_to_all(spread, SPACE, 0, 0, tiled=True)
    own = jnp.transpose(got, (3, 1, 0, 2, 4)).reshape(ROWS, 5, 32, 128)
    ahead = [(HOLDER[i], HOLDER[i + 1]) for i in range(15)]
    back = [(b, a) for a, b in ahead]
    ahead2 = [(HOLDER[i], HOLDER[i + 2]) for i in range(14)]
    back2 = [(b, a) for a, b in ahead2]
    left1 = lax.ppermute(own, TM, ahead)
    right1 = lax.ppermute(own, TM, back)
    left2 = lax.ppermute(own[ROWS - FAR :], TM, ahead2)
    right2 = lax.ppermute(own[:FAR], TM, back2)
    window = pltpu.VMEM((WINDOW, 4, 32, 128), jnp.float32)
    solved = pl.pallas_call(
        sweep_kernel,
        out_shape=f32(ROWS, 4, 32, 128),
        scratch_shapes=[window, window, window, window],
        name="sweeps",
    )(left2, left1, own, right1, right2)
    solved = jnp.transpose(solved.reshape(ROWS, 4, 16, 2, 128), (2, 1, 3, 0, 4))
    by_freq = lax.all_to_all(solved, SPACE, 0, 0, tiled=True)
    by_time = pl.pallas_call(
        backward_kernel, out_shape=f32(16, 2, 2, 2, ROWS, 128), name="backward"
    )(by_freq)
    final = lax.all_to_all(by_time, TM, 0, 0, tiled=True)
    final = jnp.stack([final[HOLDER[p]] for p in range(16)], axis=3).reshape(2, 2, 2, 128, 128)
    return final[0], final[1]


def solution(mesh):
    split = Mesh(mesh.devices.reshape(4, 2, 2, 4, 4), TM + SPACE)
    field = P(TM, SPACE, None, None)
    return jax.shard_map(
        body,
        mesh=split,
        in_specs=(field, field, P(SPACE, None, None)),
        out_specs=(field, field),
        check_vma=False,
    )
```

```python
import math

import jax
import jax.numpy as jnp
from jax import lax
from jax.experimental import pallas as pl
from jax.experimental.pallas import tpu as pltpu
from jax.sharding import Mesh
from jax.sharding import PartitionSpec as P

STEPS = 32
SWEEPS = 12
ALPHA = 0.1
MU = 1.0
BETA = 1.0

TM = ("x", "zl", "core")
SPACE = ("zh", "y")
FREQ = ("zh", "y", "core")

HALO = SWEEPS - 1
ROWS = 8
BLOCK = 2 * ROWS
WINDOW = BLOCK + 2 * HALO
PADDED = 40
VMEM = 12 << 20


def place_of(ix, zl):
    return 2 * ix + (zl + ix) % 2


PLACE = [2 * place_of(i // 4, (i // 2) % 2) + i % 2 for i in range(16)]
HOLDER = [PLACE.index(p) for p in range(16)]


def my_place():
    return place_of(lax.axis_index("x"), lax.axis_index("zl"))


def my_freq():
    return lax.axis_index("zh") * 8 + lax.axis_index("y") * 2 + lax.axis_index("core")


def add(a, b):
    return a[0] + b[0], a[1] + b[1]


def sub(a, b):
    return a[0] - b[0], a[1] - b[1]


def turned(a, k, n, sign):
    re, im = a
    if k == 0:
        return a
    if 4 * k == n:
        return (-im, re) if sign > 0 else (im, -re)
    if 8 * k == n:
        h = math.sqrt(0.5)
        return (h * (re - im), h * (im + re)) if sign > 0 else (h * (re + im), h * (im - re))
    if 8 * k == 3 * n:
        h = math.sqrt(0.5)
        return (-h * (re + im), h * (re - im)) if sign > 0 else (h * (im - re), -h * (re + im))
    c = math.cos(2.0 * math.pi * k / n)
    s = sign * math.sin(2.0 * math.pi * k / n)
    return c * re - s * im, c * im + s * re


def fourier(values, sign):
    n = len(values)
    if n == 1:
        return values
    even = fourier(values[0::2], sign)
    odd = fourier(values[1::2], sign)
    odd = [turned(odd[k], k, n, sign) for k in range(n // 2)]
    return [add(e, o) for e, o in zip(even, odd)] + [sub(e, o) for e, o in zip(even, odd)]


def growth(n):
    return math.exp(math.log(ALPHA) * n / STEPS)


def forward_kernel(times, out):
    for z in range(2):
        values = [
            (
                times[n // 2, 0, n % 2, z] * growth(n),
                times[(31 - n) // 2, 1, (31 - n) % 2, z] * growth(n),
            )
            for n in range(STEPS)
        ]
        hat = fourier(values, -1)
        for k in range(STEPS):
            out[k, 0, z] = hat[k][0]
            out[k, 1, z] = hat[k][1]


def backward_kernel(solved, out):
    for z in range(2):
        values = [(solved[k, 0, z], solved[k, 1, z]) for k in range(STEPS)]
        back = fourier(values, 1)
        for n in range(STEPS):
            scale = 1.0 / (growth(n) * STEPS)
            out[n // 2, 0, n % 2, z] = back[n][0] * scale
            out[(31 - n) // 2, 1, (31 - n) % 2, z] = back[n][1] * scale


def planes_to_rows_kernel(got, out):
    for half in range(2):
        for c in range(2):
            for j in range(4):
                tiles = got[:, j // 2, half, c, j % 2]
                out[ROWS * half : ROWS * half + ROWS, c, j] = jnp.swapaxes(tiles, 0, 1)


def rows_to_planes_kernel(solved, out):
    for half in range(2):
        for c in range(2):
            for j in range(4):
                tiles = solved[ROWS * half : ROWS * half + ROWS, c, j]
                out[:, j // 2, half, c, j % 2] = jnp.swapaxes(tiles, 0, 1)


def coefficient_kernel(reaction, coef):
    rate = math.exp(math.log(ALPHA) / STEPS)
    freq = my_freq()
    cos, sin = jnp.float32(1.0), jnp.float32(0.0)
    for k in range(1, STEPS):
        cos = jnp.where(freq == k, jnp.float32(math.cos(2.0 * math.pi * k / STEPS)), cos)
        sin = jnp.where(freq == k, jnp.float32(math.sin(2.0 * math.pi * k / STEPS)), sin)
    shift_re = 1.0 - rate * cos + 6.0 * MU
    d_im = BETA + rate * sin
    start = my_place() * BLOCK - HALO
    for j in range(4):
        for first in range(0, PADDED, ROWS):
            tiles = reaction[:, j // 2, j % 2, first : first + ROWS]
            d_re = MU * jnp.swapaxes(tiles, 0, 1) + shift_re
            row = start + first + lax.broadcasted_iota(jnp.int32, (ROWS, 8, 128), 0)
            inside = jnp.logical_and(row >= 0, row < 16 * ROWS)
            scale = jnp.where(inside, 1.0, 0.0) / (d_re * d_re + d_im * d_im)
            coef[first : first + ROWS, 0, j] = d_re * scale
            coef[first : first + ROWS, 1, j] = -d_im * scale


def sweep_kernel(left, own, right, coef, out, src, u0, u1):
    def prepare(ref, ref_row, row):
        for j in range(4):
            g_re, g_im = coef[row, 0, j], coef[row, 1, j]
            re, im = ref[ref_row, 0, j], ref[ref_row, 1, j]
            src[row, 0, j] = re
            src[row, 1, j] = im
            u0[row, 0, j] = g_re * re - g_im * im
            u0[row, 1, j] = g_re * im + g_im * re

    def spread(ref, first, count):
        def step(i, carry):
            prepare(ref, i, first + i)
            return carry

        lax.fori_loop(0, count, step, 0)

    spread(left, 0, HALO)
    spread(own, HALO, BLOCK)
    spread(right, HALO + BLOCK, HALO)

    lane = lax.broadcasted_iota(jnp.int32, (8, 128), 1)
    sublane = lax.broadcasted_iota(jnp.int32, (8, 128), 0)
    first_lane, last_lane = lane == 0, lane == 127
    first_sub, last_sub = sublane == 0, sublane == 7
    zero = jnp.zeros((8, 128), jnp.float32)

    def total(old, row, c):
        tiles = [old[row, c, j] for j in range(4)]
        below = [jnp.where(first_sub, zero, pltpu.roll(tiles[3], 1, 0))] + tiles[:3]
        above = tiles[1:] + [jnp.where(last_sub, zero, pltpu.roll(tiles[0], 7, 0))]
        sums = []
        for j in range(4):
            sides = jnp.where(first_lane, zero, pltpu.roll(tiles[j], 1, 1))
            sides = sides + jnp.where(last_lane, zero, pltpu.roll(tiles[j], 127, 1))
            outer = old[row - 1, c, j] + old[row + 1, c, j]
            sums.append(src[row, c, j] + MU * (((below[j] + above[j]) + outer) + sides))
        return sums

    for m in range(1, SWEEPS):
        old, new = (u0, u1) if m % 2 else (u1, u0)
        for row in range(m, WINDOW - m):
            s_re, s_im = total(old, row, 0), total(old, row, 1)
            for j in range(4):
                g_re, g_im = coef[row, 0, j], coef[row, 1, j]
                re = g_re * s_re[j] - g_im * s_im[j]
                im = g_re * s_im[j] + g_im * s_re[j]
                if m < SWEEPS - 1:
                    new[row, 0, j] = re
                    new[row, 1, j] = im
                else:
                    out[row - HALO, 0, j] = re
                    out[row - HALO, 1, j] = im


def call(kernel, shape, *args, scratch=()):
    return pl.pallas_call(
        kernel,
        out_shape=pltpu.VMEM(shape, jnp.float32),
        scratch_shapes=scratch,
        name=kernel.__name__,
        compiler_params=pltpu.CompilerParams(vmem_limit_bytes=VMEM),
    )(*[pltpu.with_memory_space_constraint(a, pltpu.VMEM) for a in args])


def body(state_rhs, adjoint_rhs, reaction):
    near = jnp.pad(reaction, ((0, 0), (HALO, PADDED - BLOCK - HALO), (0, 0)))
    near = lax.dynamic_slice_in_dim(near, my_place() * BLOCK, PADDED, axis=1)
    near = lax.all_to_all(jnp.broadcast_to(near, (16,) + near.shape), SPACE, 0, 0, tiled=True)
    coef = call(
        coefficient_kernel, (PADDED, 2, 4, 8, 128), near.reshape(8, 2, 2, PADDED, 128)
    )

    both = jnp.stack((state_rhs, adjoint_rhs)).reshape(2, 2, 2, 16, ROWS, 128)
    both = jnp.stack([both[:, :, :, p] for p in PLACE])
    times = lax.all_to_all(both, TM, 0, 0, tiled=True)
    hat = call(forward_kernel, (STEPS, 2, 2, ROWS, 128), times)
    got = lax.all_to_all(hat, FREQ, 0, 0, tiled=True)
    own = call(
        planes_to_rows_kernel, (BLOCK, 2, 4, 8, 128), got.reshape(8, 2, 2, 2, 2, ROWS, 128)
    )
    chain = [[HOLDER[2 * i + core] for i in range(8)] for core in range(2)]
    ahead = [(c[i], c[i + 1]) for c in chain for i in range(7)]
    left = lax.ppermute(own[BLOCK - HALO :], TM, ahead)
    right = lax.ppermute(own[:HALO], TM, [(b, a) for a, b in ahead])
    window = pltpu.VMEM((WINDOW, 2, 4, 8, 128), jnp.float32)
    solved = call(
        sweep_kernel, (BLOCK, 2, 4, 8, 128), left, own, right, coef, scratch=[window] * 3
    )
    solved = call(rows_to_planes_kernel, (8, 2, 2, 2, 2, ROWS, 128), solved)
    by_freq = lax.all_to_all(
        solved.reshape(STEPS, 2, 2, ROWS, 128), FREQ, 0, 0, tiled=True
    )
    by_time = call(backward_kernel, (16, 2, 2, 2, ROWS, 128), by_freq)
    final = lax.all_to_all(by_time, TM, 0, 0, tiled=True)
    final = jnp.stack([final[HOLDER[p]] for p in range(16)], axis=3).reshape(2, 2, 2, 128, 128)
    return final[0], final[1]


def solution(mesh):
    split = Mesh(mesh.devices.reshape(4, 2, 2, 4, 4), TM + SPACE)
    field = P(TM, SPACE, None, None)
    return jax.shard_map(
        body,
        mesh=split,
        in_specs=(field, field, P(SPACE, None, None)),
        out_specs=(field, field),
        check_vma=False,
    )
```

```python
import math

import jax
import jax.numpy as jnp
from jax import lax
from jax.experimental import pallas as pl
from jax.experimental.pallas import tpu as pltpu
from jax.sharding import Mesh
from jax.sharding import PartitionSpec as P


STEPS = 32
SWEEPS = 12
ALPHA = 0.1
MU = 1.0
BETA = 1.0

TM = ("x", "zl", "core")
SPACE = ("zh", "y")
FREQ = ("zh", "y", "core")

HALO = SWEEPS - 1
ROWS = 8
BLOCK = 2 * ROWS
WINDOW = BLOCK + 2 * HALO
PADDED = 40
VMEM = 12 << 20


def place_of(ix, zl):
    return 2 * ix + (zl + ix) % 2


PLACE = [2 * place_of(i // 4, (i // 2) % 2) + i % 2 for i in range(16)]
HOLDER = [PLACE.index(p) for p in range(16)]


def my_place():
    return place_of(lax.axis_index("x"), lax.axis_index("zl"))


def my_freq():
    return lax.axis_index("zh") * 8 + lax.axis_index("y") * 2 + lax.axis_index("core")


def add(a, b):
    return a[0] + b[0], a[1] + b[1]


def sub(a, b):
    return a[0] - b[0], a[1] - b[1]


def turned(a, k, n, sign):
    re, im = a
    if k == 0:
        return a
    if 4 * k == n:
        return (-im, re) if sign > 0 else (im, -re)
    if 8 * k == n:
        h = math.sqrt(0.5)
        return (h * (re - im), h * (im + re)) if sign > 0 else (h * (re + im), h * (im - re))
    if 8 * k == 3 * n:
        h = math.sqrt(0.5)
        return (-h * (re + im), h * (re - im)) if sign > 0 else (h * (im - re), -h * (re + im))
    c = math.cos(2.0 * math.pi * k / n)
    s = sign * math.sin(2.0 * math.pi * k / n)
    return c * re - s * im, c * im + s * re


def fourier(values, sign):
    n = len(values)
    if n == 1:
        return values
    even = fourier(values[0::2], sign)
    odd = fourier(values[1::2], sign)
    odd = [turned(odd[k], k, n, sign) for k in range(n // 2)]
    return [add(e, o) for e, o in zip(even, odd)] + [sub(e, o) for e, o in zip(even, odd)]


def growth(n):
    return math.exp(math.log(ALPHA) * n / STEPS)


def copy_all(pairs, sems):
    copies = [pltpu.make_async_copy(a, b, sems.at[n]) for n, (a, b) in enumerate(pairs)]
    for copy in copies:
        copy.start()
    for copy in copies:
        copy.wait()


def block_of(field, i):
    return field.at[:, :, ROWS * PLACE[i] : ROWS * PLACE[i] + ROWS, :]


def pack_kernel(state, adjoint, out, sems):
    fields = (state, adjoint)
    copy_all([(block_of(fields[f], i), out.at[i, f]) for i in range(16) for f in range(2)], sems)


def unpack_kernel(blocks, state, adjoint, sems):
    fields = (state, adjoint)
    copy_all([(blocks.at[i, f], block_of(fields[f], i)) for i in range(16) for f in range(2)], sems)


def forward_kernel(times, out):
    for z in range(2):
        values = [
            (
                times[n // 2, 0, n % 2, z] * growth(n),
                times[(31 - n) // 2, 1, (31 - n) % 2, z] * growth(n),
            )
            for n in range(STEPS)
        ]
        hat = fourier(values, -1)
        for k in range(STEPS):
            out[k, 0, z] = hat[k][0]
            out[k, 1, z] = hat[k][1]


def backward_kernel(solved, out):
    for z in range(2):
        values = [(solved[k, 0, z], solved[k, 1, z]) for k in range(STEPS)]
        back = fourier(values, 1)
        for n in range(STEPS):
            scale = 1.0 / (growth(n) * STEPS)
            out[n // 2, 0, n % 2, z] = back[n][0] * scale
            out[(31 - n) // 2, 1, (31 - n) % 2, z] = back[n][1] * scale


def planes_to_rows_kernel(got, out):
    for half in range(2):
        for c in range(2):
            for j in range(4):
                tiles = got[:, j // 2, half, c, j % 2]
                out[ROWS * half : ROWS * half + ROWS, c, j] = jnp.swapaxes(tiles, 0, 1)


def rows_to_planes_kernel(solved, out):
    for half in range(2):
        for c in range(2):
            for j in range(4):
                tiles = solved[ROWS * half : ROWS * half + ROWS, c, j]
                out[:, j // 2, half, c, j % 2] = jnp.swapaxes(tiles, 0, 1)


def table_of(freq, function):
    value = jnp.float32(function(0.0))
    for k in range(1, STEPS):
        value = jnp.where(freq == k, jnp.float32(function(2.0 * math.pi * k / STEPS)), value)
    return value


RATE = math.exp(math.log(ALPHA) / STEPS)


def real_kernel(out):
    value = 1.0 - RATE * table_of(my_freq(), math.cos) + 6.0 * MU
    out[...] = jnp.zeros((8, 128), jnp.float32) + value


def imaginary_kernel(out):
    value = BETA + RATE * table_of(my_freq(), math.sin)
    out[...] = jnp.zeros((8, 128), jnp.float32) + value


def coefficient_kernel(mine, other, real, imaginary, coef):
    core, zh, y = lax.axis_index("core"), lax.axis_index("zh"), lax.axis_index("y")
    shift_re, d_im = real[...], imaginary[...]
    start = my_place() * BLOCK - HALO
    for j in range(4):
        for first in range(0, PADDED, ROWS):
            at = slice(first, first + ROWS)
            tiles = []
            for slab in range(8):
                pair = 2 * slab + j // 2
                back_zh, back_y = (zh + 4 - pair // 4) % 4, (y + 4 - pair % 4) % 4
                a, b = mine[back_y, back_zh, at], other[back_y, back_zh, at]
                tiles.append(jnp.where(core == j % 2, a, b))
            d_re = MU * jnp.swapaxes(jnp.stack(tiles), 0, 1) + shift_re
            row = start + first + lax.broadcasted_iota(jnp.int32, (ROWS, 8, 128), 0)
            inside = jnp.logical_and(row >= 0, row < 16 * ROWS)
            scale = jnp.where(inside, 1.0, 0.0) / (d_re * d_re + d_im * d_im)
            coef[first : first + ROWS, 0, j] = d_re * scale
            coef[first : first + ROWS, 1, j] = -d_im * scale


def sweep_kernel(left, own, right, coef, out, src, u0, u1):
    def prepare(ref, ref_row, row):
        for j in range(4):
            g_re, g_im = coef[row, 0, j], coef[row, 1, j]
            re, im = ref[ref_row, 0, j], ref[ref_row, 1, j]
            src[row, 0, j] = re
            src[row, 1, j] = im
            u0[row, 0, j] = g_re * re - g_im * im
            u0[row, 1, j] = g_re * im + g_im * re

    def spread(ref, first, count):
        def step(i, carry):
            prepare(ref, i, first + i)
            return carry

        lax.fori_loop(0, count, step, 0)

    spread(left, 0, HALO)
    spread(own, HALO, BLOCK)
    spread(right, HALO + BLOCK, HALO)

    lane = lax.broadcasted_iota(jnp.int32, (8, 128), 1)
    sublane = lax.broadcasted_iota(jnp.int32, (8, 128), 0)
    first_lane, last_lane = lane == 0, lane == 127
    first_sub, last_sub = sublane == 0, sublane == 7
    zero = jnp.zeros((8, 128), jnp.float32)

    def total(old, row, c):
        tiles = [old[row, c, j] for j in range(4)]
        below = [jnp.where(first_sub, zero, pltpu.roll(tiles[3], 1, 0))] + tiles[:3]
        above = tiles[1:] + [jnp.where(last_sub, zero, pltpu.roll(tiles[0], 7, 0))]
        sums = []
        for j in range(4):
            sides = jnp.where(first_lane, zero, pltpu.roll(tiles[j], 1, 1))
            sides = sides + jnp.where(last_lane, zero, pltpu.roll(tiles[j], 127, 1))
            outer = old[row - 1, c, j] + old[row + 1, c, j]
            sums.append(src[row, c, j] + MU * (((below[j] + above[j]) + outer) + sides))
        return sums

    for m in range(1, SWEEPS):
        old, new = (u0, u1) if m % 2 else (u1, u0)
        for row in range(m, WINDOW - m):
            s_re, s_im = total(old, row, 0), total(old, row, 1)
            for j in range(4):
                g_re, g_im = coef[row, 0, j], coef[row, 1, j]
                re = g_re * s_re[j] - g_im * s_im[j]
                im = g_re * s_im[j] + g_im * s_re[j]
                if m < SWEEPS - 1:
                    new[row, 0, j] = re
                    new[row, 1, j] = im
                else:
                    out[row - HALO, 0, j] = re
                    out[row - HALO, 1, j] = im


def call(kernel, shape, *args, scratch=()):
    return pl.pallas_call(
        kernel,
        out_shape=pltpu.VMEM(shape, jnp.float32),
        scratch_shapes=scratch,
        compiler_params=pltpu.CompilerParams(vmem_limit_bytes=VMEM),
    )(*[pltpu.with_memory_space_constraint(a, pltpu.VMEM) for a in args])


def near_reaction(reaction):
    near = jnp.pad(reaction, ((0, 0), (HALO, PADDED - BLOCK - HALO), (0, 0)))
    first = (lax.axis_index("core"), my_place() * BLOCK, 0)
    return lax.dynamic_slice(near, first, (1, PADDED, 128))[0]


def gathered(x, axis):
    others = [lax.ppermute(x, axis, [(i, (i + d) % 4) for i in range(4)]) for d in (1, 2, 3)]
    return jnp.stack([x] + others)


def exchange(x, axes):
    return lax.all_to_all(x, axes, 0, 0, tiled=True)


def stages(state_rhs, adjoint_rhs, reaction):
    sems = pltpu.SemaphoreType.DMA((32,))
    both = pl.pallas_call(
        pack_kernel,
        in_specs=[pl.BlockSpec(memory_space=pltpu.HBM)] * 2,
        out_shape=pltpu.VMEM((16, 2, 2, 2, ROWS, 128), jnp.float32),
        scratch_shapes=[sems],
        compiler_params=pltpu.CompilerParams(vmem_limit_bytes=VMEM),
        name="pack_kernel",
    )(*[pltpu.with_memory_space_constraint(a, pltpu.HBM) for a in (state_rhs, adjoint_rhs)])
    times = exchange(both, TM)
    mine = gathered(gathered(near_reaction(reaction), "zh"), "y")
    other = lax.ppermute(mine, "core", [(0, 1), (1, 0)])
    real, imaginary = call(real_kernel, (8, 128)), call(imaginary_kernel, (8, 128))
    coef = call(coefficient_kernel, (PADDED, 2, 4, 8, 128), mine, other, real, imaginary)
    hat = call(forward_kernel, (STEPS, 2, 2, ROWS, 128), times)
    got = exchange(hat, FREQ)
    own = call(
        planes_to_rows_kernel, (BLOCK, 2, 4, 8, 128), got.reshape(8, 2, 2, 2, 2, ROWS, 128)
    )
    chain = [[HOLDER[2 * i + core] for i in range(8)] for core in range(2)]
    ahead = [(c[i], c[i + 1]) for c in chain for i in range(7)]
    left = lax.ppermute(own[BLOCK - HALO :], TM, ahead)
    right = lax.ppermute(own[:HALO], TM, [(b, a) for a, b in ahead])
    window = pltpu.VMEM((WINDOW, 2, 4, 8, 128), jnp.float32)
    solved = call(
        sweep_kernel, (BLOCK, 2, 4, 8, 128), left, own, right, coef, scratch=[window] * 3
    )
    solved = call(rows_to_planes_kernel, (8, 2, 2, 2, 2, ROWS, 128), solved)
    by_freq = exchange(solved.reshape(STEPS, 2, 2, ROWS, 128), FREQ)
    by_time = call(backward_kernel, (16, 2, 2, 2, ROWS, 128), by_freq)
    final = exchange(by_time, TM)
    return pl.pallas_call(
        unpack_kernel,
        out_specs=[pl.BlockSpec(memory_space=pltpu.HBM)] * 2,
        out_shape=[jax.ShapeDtypeStruct(state_rhs.shape, jnp.float32)] * 2,
        scratch_shapes=[sems],
        compiler_params=pltpu.CompilerParams(vmem_limit_bytes=VMEM),
        name="unpack_kernel",
    )(pltpu.with_memory_space_constraint(final, pltpu.VMEM))


def solution(mesh):
    split = Mesh(mesh.devices.reshape(4, 2, 2, 4, 4), TM + SPACE)
    field = P(TM, SPACE, None, None)
    return jax.shard_map(
        stages,
        mesh=split,
        in_specs=(field, field, P(SPACE, None, None)),
        out_specs=(field, field),
        check_vma=False,
    )
```

```python
import math

import jax
import jax.numpy as jnp
from jax import lax
from jax.experimental import pallas as pl
from jax.experimental.pallas import tpu as pltpu
from jax.sharding import Mesh
from jax.sharding import PartitionSpec as P


STEPS = 32
SWEEPS = 12
ALPHA = 0.1
MU = 1.0
BETA = 1.0

TM = ("x", "zl", "core")
SPACE = ("zh", "y")
TIME = ("core", "x", "zl")
FREQ = ("zl", "y", "zh")

HALO = SWEEPS - 1
ROWS = 8
BLOCK = 2 * ROWS
WINDOW = BLOCK + 2 * HALO
PADDED = 40
NEAR = PADDED + BLOCK
VMEM = 12 << 20


def place_of(ix, core):
    return 2 * ix + (core + ix) % 2


def device_of(place, zl):
    ix = place // 2
    return 4 * ix + 2 * zl + (place + ix) % 2


TIME_TO_TM = [4 * ((e // 2) % 4) + 2 * (e % 2) + e // 8 for e in range(16)]
TM_TO_TIME = [TIME_TO_TM.index(i) for i in range(16)]
PLACE = [2 * place_of((e // 2) % 4, e // 8) + e % 2 for e in range(16)]


def my_place():
    return place_of(lax.axis_index("x"), lax.axis_index("core"))


def my_freq():
    return lax.axis_index("zl") * 16 + lax.axis_index("y") * 4 + lax.axis_index("zh")


def add(a, b):
    return a[0] + b[0], a[1] + b[1]


def sub(a, b):
    return a[0] - b[0], a[1] - b[1]


def turned(a, k, n, sign):
    re, im = a
    if k == 0:
        return a
    if 4 * k == n:
        return (-im, re) if sign > 0 else (im, -re)
    if 8 * k == n:
        h = math.sqrt(0.5)
        return (h * (re - im), h * (im + re)) if sign > 0 else (h * (re + im), h * (im - re))
    if 8 * k == 3 * n:
        h = math.sqrt(0.5)
        return (-h * (re + im), h * (re - im)) if sign > 0 else (h * (im - re), -h * (re + im))
    c = math.cos(2.0 * math.pi * k / n)
    s = sign * math.sin(2.0 * math.pi * k / n)
    return c * re - s * im, c * im + s * re


def fourier(values, sign):
    n = len(values)
    if n == 1:
        return values
    even = fourier(values[0::2], sign)
    odd = fourier(values[1::2], sign)
    odd = [turned(odd[k], k, n, sign) for k in range(n // 2)]
    return [add(e, o) for e, o in zip(even, odd)] + [sub(e, o) for e, o in zip(even, odd)]


def growth(n):
    return math.exp(math.log(ALPHA) * n / STEPS)


def copy_all(pairs, sems):
    copies = [pltpu.make_async_copy(a, b, sems.at[n]) for n, (a, b) in enumerate(pairs)]
    for copy in copies:
        copy.start()
    for copy in copies:
        copy.wait()


def block_of(field, i):
    return field.at[:, :, ROWS * PLACE[i] : ROWS * PLACE[i] + ROWS, :]


def pack_kernel(state, adjoint, out, sems):
    fields = (state, adjoint)
    copy_all([(block_of(fields[f], i), out.at[i, f]) for i in range(16) for f in range(2)], sems)


def unpack_kernel(blocks, state, adjoint, sems):
    fields = (state, adjoint)
    copy_all([(blocks.at[i, f], block_of(fields[f], i)) for i in range(16) for f in range(2)], sems)


def forward_kernel(times, out):
    def time(field, n, z):
        return times[TM_TO_TIME[n // 2], field, n % 2, z]

    for z in range(2):
        values = [
            (time(0, n, z) * growth(n), time(1, 31 - n, z) * growth(n)) for n in range(STEPS)
        ]
        hat = fourier(values, -1)
        for k in range(STEPS):
            out[k, 0, z] = hat[k][0]
            out[k, 1, z] = hat[k][1]


def backward_kernel(solved, out):
    for z in range(2):
        values = [(solved[k, 0, z], solved[k, 1, z]) for k in range(STEPS)]
        back = fourier(values, 1)
        for n in range(STEPS):
            scale = 1.0 / (growth(n) * STEPS)
            out[TM_TO_TIME[n // 2], 0, n % 2, z] = back[n][0] * scale
            out[TM_TO_TIME[(31 - n) // 2], 1, (31 - n) % 2, z] = back[n][1] * scale


def planes_to_rows_kernel(got, out):
    for half in range(2):
        for c in range(2):
            for j in range(4):
                tiles = [got[half, q % 2, j // 2, q // 2, c, j % 2] for q in range(8)]
                at = slice(ROWS * half, ROWS * half + ROWS)
                out[at, c, j] = jnp.swapaxes(jnp.stack(tiles), 0, 1)


def rows_to_planes_kernel(solved, out):
    for half in range(2):
        for c in range(2):
            for j in range(4):
                at = slice(ROWS * half, ROWS * half + ROWS)
                tiles = jnp.swapaxes(solved[at, c, j], 0, 1)
                for q in range(8):
                    out[half, q % 2, j // 2, q // 2, c, j % 2] = tiles[q]


def table_of(freq, function):
    value = jnp.float32(function(0.0))
    for k in range(1, STEPS):
        value = jnp.where(freq == k, jnp.float32(function(2.0 * math.pi * k / STEPS)), value)
    return value


RATE = math.exp(math.log(ALPHA) / STEPS)


def real_kernel(out):
    value = 1.0 - RATE * table_of(my_freq(), math.cos) + 6.0 * MU
    out[...] = jnp.zeros((8, 128), jnp.float32) + value


def imaginary_kernel(out):
    value = BETA + RATE * table_of(my_freq(), math.sin)
    out[...] = jnp.zeros((8, 128), jnp.float32) + value


def coefficient_kernel(mine, other, real, imaginary, coef):
    core, zh, y = lax.axis_index("core"), lax.axis_index("zh"), lax.axis_index("y")
    shift_re, d_im = real[...], imaginary[...]
    start = my_place() * BLOCK - HALO
    offset = pl.multiple_of(my_place() % 2 * BLOCK, BLOCK)
    for j in range(4):
        for first in range(0, PADDED, ROWS):
            at = pl.ds(offset + first, ROWS)
            tiles = []
            for slab in range(8):
                pair = 2 * slab + j // 2
                back_zh, back_y = (zh + 4 - pair // 4) % 4, (y + 4 - pair % 4) % 4
                a, b = mine[back_y, back_zh, at], other[back_y, back_zh, at]
                tiles.append(jnp.where(core == j % 2, a, b))
            d_re = MU * jnp.swapaxes(jnp.stack(tiles), 0, 1) + shift_re
            row = start + first + lax.broadcasted_iota(jnp.int32, (ROWS, 8, 128), 0)
            inside = jnp.logical_and(row >= 0, row < 16 * ROWS)
            scale = jnp.where(inside, 1.0, 0.0) / (d_re * d_re + d_im * d_im)
            coef[first : first + ROWS, 0, j] = d_re * scale
            coef[first : first + ROWS, 1, j] = -d_im * scale


def sweep_kernel(left, own, right, coef, out, src, u0, u1):
    def prepare(ref, ref_row, row):
        for j in range(4):
            g_re, g_im = coef[row, 0, j], coef[row, 1, j]
            re, im = ref[ref_row, 0, j], ref[ref_row, 1, j]
            src[row, 0, j] = re
            src[row, 1, j] = im
            u0[row, 0, j] = g_re * re - g_im * im
            u0[row, 1, j] = g_re * im + g_im * re

    def spread(ref, first, count):
        def step(i, carry):
            prepare(ref, i, first + i)
            return carry

        lax.fori_loop(0, count, step, 0)

    spread(left, 0, HALO)
    spread(own, HALO, BLOCK)
    spread(right, HALO + BLOCK, HALO)

    lane = lax.broadcasted_iota(jnp.int32, (8, 128), 1)
    sublane = lax.broadcasted_iota(jnp.int32, (8, 128), 0)
    first_lane, last_lane = lane == 0, lane == 127
    first_sub, last_sub = sublane == 0, sublane == 7
    zero = jnp.zeros((8, 128), jnp.float32)

    def total(old, row, c):
        tiles = [old[row, c, j] for j in range(4)]
        below = [jnp.where(first_sub, zero, pltpu.roll(tiles[3], 1, 0))] + tiles[:3]
        above = tiles[1:] + [jnp.where(last_sub, zero, pltpu.roll(tiles[0], 7, 0))]
        sums = []
        for j in range(4):
            sides = jnp.where(first_lane, zero, pltpu.roll(tiles[j], 1, 1))
            sides = sides + jnp.where(last_lane, zero, pltpu.roll(tiles[j], 127, 1))
            outer = old[row - 1, c, j] + old[row + 1, c, j]
            sums.append(src[row, c, j] + MU * (((below[j] + above[j]) + outer) + sides))
        return sums

    for m in range(1, SWEEPS):
        old, new = (u0, u1) if m % 2 else (u1, u0)
        for row in range(m, WINDOW - m):
            s_re, s_im = total(old, row, 0), total(old, row, 1)
            for j in range(4):
                g_re, g_im = coef[row, 0, j], coef[row, 1, j]
                re = g_re * s_re[j] - g_im * s_im[j]
                im = g_re * s_im[j] + g_im * s_re[j]
                if m < SWEEPS - 1:
                    new[row, 0, j] = re
                    new[row, 1, j] = im
                else:
                    out[row - HALO, 0, j] = re
                    out[row - HALO, 1, j] = im


def call(kernel, shape, *args, scratch=()):
    return pl.pallas_call(
        kernel,
        out_shape=pltpu.VMEM(shape, jnp.float32),
        scratch_shapes=scratch,
        compiler_params=pltpu.CompilerParams(vmem_limit_bytes=VMEM),
    )(*[pltpu.with_memory_space_constraint(a, pltpu.VMEM) for a in args])


def near_reaction(reaction):
    near = jnp.pad(reaction, ((0, 0), (HALO, NEAR - 2 * BLOCK - HALO), (0, 0)))
    first = (lax.axis_index("core"), lax.axis_index("x") * 2 * BLOCK, 0)
    return lax.dynamic_slice(near, first, (1, NEAR, 128))[0]


def gathered(x, axis):
    others = [lax.ppermute(x, axis, [(i, (i + d) % 4) for i in range(4)]) for d in (1, 2, 3)]
    return jnp.stack([x] + others)


def exchange(x, axes):
    return lax.all_to_all(x, axes, 0, 0, tiled=True)


def stages(state_rhs, adjoint_rhs, reaction):
    sems = pltpu.SemaphoreType.DMA((32,))
    both = pl.pallas_call(
        pack_kernel,
        in_specs=[pl.BlockSpec(memory_space=pltpu.HBM)] * 2,
        out_shape=pltpu.VMEM((16, 2, 2, 2, ROWS, 128), jnp.float32),
        scratch_shapes=[sems],
        compiler_params=pltpu.CompilerParams(vmem_limit_bytes=VMEM),
        name="pack_kernel",
    )(*[pltpu.with_memory_space_constraint(a, pltpu.HBM) for a in (state_rhs, adjoint_rhs)])
    times = exchange(both, TIME)
    mine = gathered(gathered(near_reaction(reaction), "zh"), "y")
    other = lax.ppermute(mine, "core", [(0, 1), (1, 0)])
    real, imaginary = call(real_kernel, (8, 128)), call(imaginary_kernel, (8, 128))
    coef = call(coefficient_kernel, (PADDED, 2, 4, 8, 128), mine, other, real, imaginary)
    hat = call(forward_kernel, (STEPS, 2, 2, ROWS, 128), times)
    got = exchange(hat, FREQ)
    got = got.reshape(2, 2, 2, 4, 2, 2, ROWS, 128)
    own = call(planes_to_rows_kernel, (BLOCK, 2, 4, 8, 128), got)
    ahead = [(device_of(i, zl), device_of(i + 1, zl)) for zl in range(2) for i in range(7)]
    left = lax.ppermute(own[BLOCK - HALO :], TM, ahead)
    right = lax.ppermute(own[:HALO], TM, [(b, a) for a, b in ahead])
    window = pltpu.VMEM((WINDOW, 2, 4, 8, 128), jnp.float32)
    solved = call(
        sweep_kernel, (BLOCK, 2, 4, 8, 128), left, own, right, coef, scratch=[window] * 3
    )
    solved = call(rows_to_planes_kernel, (2, 2, 2, 4, 2, 2, ROWS, 128), solved)
    by_freq = exchange(solved.reshape(STEPS, 2, 2, ROWS, 128), FREQ)
    by_time = call(backward_kernel, (16, 2, 2, 2, ROWS, 128), by_freq)
    final = exchange(by_time, TIME)
    return pl.pallas_call(
        unpack_kernel,
        out_specs=[pl.BlockSpec(memory_space=pltpu.HBM)] * 2,
        out_shape=[jax.ShapeDtypeStruct(state_rhs.shape, jnp.float32)] * 2,
        scratch_shapes=[sems],
        compiler_params=pltpu.CompilerParams(vmem_limit_bytes=VMEM),
        name="unpack_kernel",
    )(pltpu.with_memory_space_constraint(final, pltpu.VMEM))


def solution(mesh):
    split = Mesh(mesh.devices.reshape(4, 2, 2, 4, 4), TM + SPACE)
    field = P(TM, SPACE, None, None)
    return jax.shard_map(
        stages,
        mesh=split,
        in_specs=(field, field, P(SPACE, None, None)),
        out_specs=(field, field),
        check_vma=False,
    )
```

```python
import math

import jax
import jax.numpy as jnp
from jax import lax
from jax.experimental import pallas as pl
from jax.experimental.pallas import tpu as pltpu
from jax.sharding import Mesh
from jax.sharding import PartitionSpec as P


STEPS = 32
SWEEPS = 12
ALPHA = 0.1
MU = 1.0
BETA = 1.0

TM = ("x", "zl", "core")
SPACE = ("zh", "y")
TIME = ("core", "x", "zl")
FREQ = ("zl", "y", "zh")

HALO = SWEEPS - 1
ROWS = 8
BLOCK = 2 * ROWS
WINDOW = BLOCK + 2 * HALO
PADDED = 40
NEAR = PADDED + BLOCK
VMEM = 12 << 20


def place_of(ix, core):
    return 2 * ix + (core + ix) % 2


def device_of(place, zl):
    ix = place // 2
    return 4 * ix + 2 * zl + (place + ix) % 2


TIME_TO_TM = [4 * ((e // 2) % 4) + 2 * (e % 2) + e // 8 for e in range(16)]
TM_TO_TIME = [TIME_TO_TM.index(i) for i in range(16)]
PLACE = [2 * place_of((e // 2) % 4, e // 8) + e % 2 for e in range(16)]


def my_place():
    return place_of(lax.axis_index("x"), lax.axis_index("core"))


def my_freq():
    return lax.axis_index("zl") * 16 + lax.axis_index("y") * 4 + lax.axis_index("zh")


def add(a, b):
    return a[0] + b[0], a[1] + b[1]


def sub(a, b):
    return a[0] - b[0], a[1] - b[1]


def turned(a, k, n, sign):
    re, im = a
    if k == 0:
        return a
    if 4 * k == n:
        return (-im, re) if sign > 0 else (im, -re)
    if 8 * k == n:
        h = math.sqrt(0.5)
        return (h * (re - im), h * (im + re)) if sign > 0 else (h * (re + im), h * (im - re))
    if 8 * k == 3 * n:
        h = math.sqrt(0.5)
        return (-h * (re + im), h * (re - im)) if sign > 0 else (h * (im - re), -h * (re + im))
    c = math.cos(2.0 * math.pi * k / n)
    s = sign * math.sin(2.0 * math.pi * k / n)
    return c * re - s * im, c * im + s * re


def fourier(values, sign):
    n = len(values)
    if n == 1:
        return values
    even = fourier(values[0::2], sign)
    odd = fourier(values[1::2], sign)
    odd = [turned(odd[k], k, n, sign) for k in range(n // 2)]
    return [add(e, o) for e, o in zip(even, odd)] + [sub(e, o) for e, o in zip(even, odd)]


def growth(n):
    return math.exp(math.log(ALPHA) * n / STEPS)


def copy_all(pairs, sems):
    copies = [pltpu.make_async_copy(a, b, sems.at[n]) for n, (a, b) in enumerate(pairs)]
    for copy in copies:
        copy.start()
    for copy in copies:
        copy.wait()


def block_of(field, i):
    return field.at[:, :, ROWS * PLACE[i] : ROWS * PLACE[i] + ROWS, :]


def pack_kernel(state, adjoint, out, sems):
    fields = (state, adjoint)
    copy_all([(block_of(fields[f], i), out.at[i, f]) for i in range(16) for f in range(2)], sems)


def unpack_kernel(blocks, state, adjoint, sems):
    fields = (state, adjoint)
    copy_all([(blocks.at[i, f], block_of(fields[f], i)) for i in range(16) for f in range(2)], sems)


def forward_kernel(times, out):
    def time(field, n, z):
        return times[TM_TO_TIME[n // 2], field, n % 2, z]

    for z in range(2):
        values = [
            (time(0, n, z) * growth(n), time(1, 31 - n, z) * growth(n)) for n in range(STEPS)
        ]
        hat = fourier(values, -1)
        for k in range(STEPS):
            out[k, 0, z] = hat[k][0]
            out[k, 1, z] = hat[k][1]


def backward_kernel(solved, out):
    for z in range(2):
        values = [(solved[k, 0, z], solved[k, 1, z]) for k in range(STEPS)]
        back = fourier(values, 1)
        for n in range(STEPS):
            scale = 1.0 / (growth(n) * STEPS)
            out[TM_TO_TIME[n // 2], 0, n % 2, z] = back[n][0] * scale
            out[TM_TO_TIME[(31 - n) // 2], 1, (31 - n) % 2, z] = back[n][1] * scale


def planes_to_rows_kernel(got, out):
    for half in range(2):
        for c in range(2):
            for j in range(4):
                tiles = [got[half, q % 2, j // 2, q // 2, c, j % 2] for q in range(8)]
                at = slice(ROWS * half, ROWS * half + ROWS)
                out[at, c, j] = jnp.swapaxes(jnp.stack(tiles), 0, 1)


def rows_to_planes_kernel(solved, out):
    for half in range(2):
        for c in range(2):
            for j in range(4):
                at = slice(ROWS * half, ROWS * half + ROWS)
                tiles = jnp.swapaxes(solved[at, c, j], 0, 1)
                for q in range(8):
                    out[half, q % 2, j // 2, q // 2, c, j % 2] = tiles[q]


def table_of(freq, function):
    value = jnp.float32(function(0.0))
    for k in range(1, STEPS):
        value = jnp.where(freq == k, jnp.float32(function(2.0 * math.pi * k / STEPS)), value)
    return value


RATE = math.exp(math.log(ALPHA) / STEPS)


def spread(out, value):
    out[...] = jnp.zeros((8, 128), jnp.float32) + value


def real_kernel(out):
    spread(out, 1.0 - RATE * table_of(my_freq(), math.cos) + 6.0 * MU)


def imaginary_kernel(out):
    spread(out, BETA + RATE * table_of(my_freq(), math.sin))


def start_kernel(out):
    spread(out, (my_place() * BLOCK - HALO).astype(jnp.float32))


def coefficient_kernel(mine, other, real, imaginary, start, coef):
    core, zh, y = lax.axis_index("core"), lax.axis_index("zh"), lax.axis_index("y")
    shift_re, d_im = real[...], imaginary[...]
    offset = pl.multiple_of(my_place() % 2 * BLOCK, BLOCK)
    for j in range(4):
        for first in range(0, PADDED, ROWS):
            at = pl.ds(offset + first, ROWS)
            tiles = []
            for slab in range(8):
                pair = 2 * slab + j // 2
                back_zh, back_y = (zh + 4 - pair // 4) % 4, (y + 4 - pair % 4) % 4
                a, b = mine[back_y, back_zh, at], other[back_y, back_zh, at]
                tiles.append(jnp.where(core == j % 2, a, b))
            d_re = MU * jnp.swapaxes(jnp.stack(tiles), 0, 1) + shift_re
            step = lax.broadcasted_iota(jnp.int32, (ROWS, 8, 128), 0).astype(jnp.float32)
            row = start[...] + (step + first)
            inside = jnp.logical_and(row >= 0.0, row < 16.0 * ROWS)
            scale = jnp.where(inside, 1.0, 0.0) / (d_re * d_re + d_im * d_im)
            coef[first : first + ROWS, 0, j] = d_re * scale
            coef[first : first + ROWS, 1, j] = -d_im * scale


def swept(get, source, coef, row, c_row):
    lane = lax.broadcasted_iota(jnp.int32, (8, 128), 1)
    sublane = lax.broadcasted_iota(jnp.int32, (8, 128), 0)
    zero = jnp.zeros((8, 128), jnp.float32)

    def total(c):
        tiles = [get(row, c, j) for j in range(4)]
        below = [jnp.where(sublane == 0, zero, pltpu.roll(tiles[3], 1, 0))] + tiles[:3]
        above = tiles[1:] + [jnp.where(sublane == 7, zero, pltpu.roll(tiles[0], 7, 0))]
        sums = []
        for j in range(4):
            sides = jnp.where(lane == 0, zero, pltpu.roll(tiles[j], 1, 1))
            sides = sides + jnp.where(lane == 127, zero, pltpu.roll(tiles[j], 127, 1))
            outer = get(row - 1, c, j) + get(row + 1, c, j)
            sums.append(source(row, c, j) + MU * (((below[j] + above[j]) + outer) + sides))
        return sums

    return times_coefficient(coef, c_row, total(0), total(1))


def times_coefficient(coef, row, s_re, s_im):
    result = []
    for j in range(4):
        g_re, g_im = coef[row, 0, j], coef[row, 1, j]
        result.append((g_re * s_re[j] - g_im * s_im[j], g_re * s_im[j] + g_im * s_re[j]))
    return result


def put(ref, at, values):
    for j in range(4):
        ref[(*at, 0, j)] = values[j][0]
        ref[(*at, 1, j)] = values[j][1]


def first_fields(ref, rows, coef, c_first, write):
    def step(i, carry):
        s_re, s_im = ([ref[i, c, j] for j in range(4)] for c in range(2))
        write(i, times_coefficient(coef, c_first + i, s_re, s_im))
        return carry

    lax.fori_loop(0, rows, step, 0)


INNER = BLOCK // 2


def inner_kernel(own, coef, levels):
    first_fields(own, BLOCK, coef, HALO, lambda i, values: put(levels, (0, i), values))
    for m in range(1, INNER):
        for row in range(m, BLOCK - m):
            values = swept(
                lambda r, c, j, m=m: levels[m - 1, r, c, j],
                lambda r, c, j: own[r, c, j],
                coef,
                row,
                row + HALO,
            )
            put(levels, (m, row), values)


def sweep_kernel(left, own, right, coef, levels, out, u0, u1):
    fields = (u0, u1)
    first_fields(left, HALO, coef, 0, lambda i, values: put(u0, (i,), values))
    behind = HALO + BLOCK
    first_fields(right, HALO, coef, behind, lambda i, values: put(u0, (behind + i,), values))

    def inside(m, row):
        return m < INNER and m <= row - HALO < BLOCK - m

    def source(row, c, j):
        if row < HALO:
            return left[row, c, j]
        return own[row - HALO, c, j] if row < behind else right[row - behind, c, j]

    def getter(m):
        def get(row, c, j):
            return levels[m, row - HALO, c, j] if inside(m, row) else fields[m % 2][row, c, j]

        return get

    for m in range(1, SWEEPS):
        for row in range(m, WINDOW - m):
            if inside(m, row):
                continue
            values = swept(getter(m - 1), source, coef, row, row)
            if m < SWEEPS - 1:
                put(fields[m % 2], (row,), values)
            else:
                put(out, (row - HALO,), values)


def call(kernel, shape, *args, scratch=()):
    return pl.pallas_call(
        kernel,
        out_shape=pltpu.VMEM(shape, jnp.float32),
        scratch_shapes=scratch,
        compiler_params=pltpu.CompilerParams(vmem_limit_bytes=VMEM),
    )(*[pltpu.with_memory_space_constraint(a, pltpu.VMEM) for a in args])


def near_reaction(reaction):
    near = jnp.pad(reaction, ((0, 0), (HALO, NEAR - 2 * BLOCK - HALO), (0, 0)))
    first = (lax.axis_index("core"), lax.axis_index("x") * 2 * BLOCK, 0)
    return lax.dynamic_slice(near, first, (1, NEAR, 128))[0]


def gathered(x, axis):
    others = [lax.ppermute(x, axis, [(i, (i + d) % 4) for i in range(4)]) for d in (1, 2, 3)]
    return jnp.stack([x] + others)


def exchange(x, axes):
    return lax.all_to_all(x, axes, 0, 0, tiled=True)


def stages(state_rhs, adjoint_rhs, reaction):
    sems = pltpu.SemaphoreType.DMA((32,))
    both = pl.pallas_call(
        pack_kernel,
        in_specs=[pl.BlockSpec(memory_space=pltpu.HBM)] * 2,
        out_shape=pltpu.VMEM((16, 2, 2, 2, ROWS, 128), jnp.float32),
        scratch_shapes=[sems],
        compiler_params=pltpu.CompilerParams(vmem_limit_bytes=VMEM),
        name="pack_kernel",
    )(*[pltpu.with_memory_space_constraint(a, pltpu.HBM) for a in (state_rhs, adjoint_rhs)])
    times = exchange(both, TIME)
    mine = gathered(gathered(near_reaction(reaction), "zh"), "y")
    other = lax.ppermute(mine, "core", [(0, 1), (1, 0)])
    shifts = [call(kernel, (8, 128)) for kernel in (real_kernel, imaginary_kernel, start_kernel)]
    coef = call(coefficient_kernel, (PADDED, 2, 4, 8, 128), mine, other, *shifts)
    hat = call(forward_kernel, (STEPS, 2, 2, ROWS, 128), times)
    got = exchange(hat, FREQ)
    got = got.reshape(2, 2, 2, 4, 2, 2, ROWS, 128)
    own = call(planes_to_rows_kernel, (BLOCK, 2, 4, 8, 128), got)
    ahead = [(device_of(i, zl), device_of(i + 1, zl)) for zl in range(2) for i in range(7)]
    left = lax.ppermute(own[BLOCK - HALO :], TM, ahead)
    right = lax.ppermute(own[:HALO], TM, [(b, a) for a, b in ahead])
    levels = call(inner_kernel, (INNER, BLOCK, 2, 4, 8, 128), own, coef)
    window = pltpu.VMEM((WINDOW, 2, 4, 8, 128), jnp.float32)
    block = (BLOCK, 2, 4, 8, 128)
    solved = call(sweep_kernel, block, left, own, right, coef, levels, scratch=[window] * 2)
    solved = call(rows_to_planes_kernel, (2, 2, 2, 4, 2, 2, ROWS, 128), solved)
    by_freq = exchange(solved.reshape(STEPS, 2, 2, ROWS, 128), FREQ)
    by_time = call(backward_kernel, (16, 2, 2, 2, ROWS, 128), by_freq)
    final = exchange(by_time, TIME)
    return pl.pallas_call(
        unpack_kernel,
        out_specs=[pl.BlockSpec(memory_space=pltpu.HBM)] * 2,
        out_shape=[jax.ShapeDtypeStruct(state_rhs.shape, jnp.float32)] * 2,
        scratch_shapes=[sems],
        compiler_params=pltpu.CompilerParams(vmem_limit_bytes=VMEM),
        name="unpack_kernel",
    )(pltpu.with_memory_space_constraint(final, pltpu.VMEM))


def solution(mesh):
    split = Mesh(mesh.devices.reshape(4, 2, 2, 4, 4), TM + SPACE)
    field = P(TM, SPACE, None, None)
    return jax.shard_map(
        stages,
        mesh=split,
        in_specs=(field, field, P(SPACE, None, None)),
        out_specs=(field, field),
        check_vma=False,
    )
```

```python
import math

import jax
import jax.numpy as jnp
from jax import lax
from jax.experimental import pallas as pl
from jax.experimental.pallas import tpu as pltpu
from jax.sharding import Mesh
from jax.sharding import PartitionSpec as P


STEPS = 32
SWEEPS = 12
ALPHA = 0.1
MU = 1.0
BETA = 1.0

TM = ("x", "zl", "core")
SPACE = ("zh", "y")
TIME = ("core", "x", "zl")
FREQ = ("zl", "y", "zh")

HALO = SWEEPS - 1
ROWS = 8
BLOCK = 2 * ROWS
WINDOW = BLOCK + 2 * HALO
PADDED = 40
NEAR = PADDED + BLOCK
VMEM = 12 << 20


def place_of(ix, core):
    return 2 * ix + (core + ix) % 2


def device_of(place, zl):
    ix = place // 2
    return 4 * ix + 2 * zl + (place + ix) % 2


TIME_TO_TM = [4 * ((e // 2) % 4) + 2 * (e % 2) + e // 8 for e in range(16)]
TM_TO_TIME = [TIME_TO_TM.index(i) for i in range(16)]
PLACE = [2 * place_of((e // 2) % 4, e // 8) + e % 2 for e in range(16)]


def my_place():
    return place_of(lax.axis_index("x"), lax.axis_index("core"))


def my_freq():
    return lax.axis_index("zl") * 16 + lax.axis_index("y") * 4 + lax.axis_index("zh")


def add(a, b):
    return a[0] + b[0], a[1] + b[1]


def sub(a, b):
    return a[0] - b[0], a[1] - b[1]


def turned(a, k, n, sign):
    re, im = a
    if k == 0:
        return a
    if 4 * k == n:
        return (-im, re) if sign > 0 else (im, -re)
    if 8 * k == n:
        h = math.sqrt(0.5)
        return (h * (re - im), h * (im + re)) if sign > 0 else (h * (re + im), h * (im - re))
    if 8 * k == 3 * n:
        h = math.sqrt(0.5)
        return (-h * (re + im), h * (re - im)) if sign > 0 else (h * (im - re), -h * (re + im))
    c = math.cos(2.0 * math.pi * k / n)
    s = sign * math.sin(2.0 * math.pi * k / n)
    return c * re - s * im, c * im + s * re


def fourier(values, sign):
    n = len(values)
    if n == 1:
        return values
    even = fourier(values[0::2], sign)
    odd = fourier(values[1::2], sign)
    odd = [turned(odd[k], k, n, sign) for k in range(n // 2)]
    return [add(e, o) for e, o in zip(even, odd)] + [sub(e, o) for e, o in zip(even, odd)]


def growth(n):
    return math.exp(math.log(ALPHA) * n / STEPS)


def copy_all(pairs, sems):
    copies = [pltpu.make_async_copy(a, b, sems.at[n]) for n, (a, b) in enumerate(pairs)]
    for copy in copies:
        copy.start()
    for copy in copies:
        copy.wait()


def block_of(field, i):
    return field.at[:, :, ROWS * PLACE[i] : ROWS * PLACE[i] + ROWS, :]


def pack_kernel(state, adjoint, out, sems):
    fields = (state, adjoint)
    copy_all([(block_of(fields[f], i), out.at[i, f]) for i in range(16) for f in range(2)], sems)


def unpack_kernel(blocks, state, adjoint, sems):
    fields = (state, adjoint)
    copy_all([(blocks.at[i, f], block_of(fields[f], i)) for i in range(16) for f in range(2)], sems)


def forward_kernel(times, out):
    def time(field, n, z):
        return times[TM_TO_TIME[n // 2], field, n % 2, z]

    for z in range(2):
        values = [
            (time(0, n, z) * growth(n), time(1, 31 - n, z) * growth(n)) for n in range(STEPS)
        ]
        hat = fourier(values, -1)
        for k in range(STEPS):
            out[k, 0, z] = hat[k][0]
            out[k, 1, z] = hat[k][1]


def backward_kernel(solved, out):
    for z in range(2):
        values = [(solved[k, 0, z], solved[k, 1, z]) for k in range(STEPS)]
        back = fourier(values, 1)
        for n in range(STEPS):
            scale = 1.0 / (growth(n) * STEPS)
            out[TM_TO_TIME[n // 2], 0, n % 2, z] = back[n][0] * scale
            out[TM_TO_TIME[(31 - n) // 2], 1, (31 - n) % 2, z] = back[n][1] * scale


def planes_to_rows_kernel(got, out):
    for half in range(2):
        for c in range(2):
            for j in range(4):
                tiles = [got[half, q % 2, j // 2, q // 2, c, j % 2] for q in range(8)]
                at = slice(ROWS * half, ROWS * half + ROWS)
                out[at, c, j] = jnp.swapaxes(jnp.stack(tiles), 0, 1)


def rows_to_planes_kernel(solved, out):
    for half in range(2):
        for c in range(2):
            for j in range(4):
                at = slice(ROWS * half, ROWS * half + ROWS)
                tiles = jnp.swapaxes(solved[at, c, j], 0, 1)
                for q in range(8):
                    out[half, q % 2, j // 2, q // 2, c, j % 2] = tiles[q]


def table_of(freq, function):
    value = jnp.float32(function(0.0))
    for k in range(1, STEPS):
        value = jnp.where(freq == k, jnp.float32(function(2.0 * math.pi * k / STEPS)), value)
    return value


RATE = math.exp(math.log(ALPHA) / STEPS)


def spread(out, value):
    out[...] = jnp.zeros((8, 128), jnp.float32) + value


def real_kernel(out):
    spread(out, 1.0 - RATE * table_of(my_freq(), math.cos) + 6.0 * MU)


def imaginary_kernel(out):
    spread(out, BETA + RATE * table_of(my_freq(), math.sin))


def start_kernel(out):
    spread(out, (my_place() * BLOCK - HALO).astype(jnp.float32))


def coefficient_kernel(mine, other, real, imaginary, start, coef):
    core, zh, y = lax.axis_index("core"), lax.axis_index("zh"), lax.axis_index("y")
    shift_re, d_im = real[...], imaginary[...]
    offset = pl.multiple_of(my_place() % 2 * BLOCK, BLOCK)
    for j in range(4):
        for first in range(0, PADDED, ROWS):
            at = pl.ds(offset + first, ROWS)
            tiles = []
            for slab in range(8):
                pair = 2 * slab + j // 2
                from_zh, from_y = lax.bitwise_xor(zh, pair // 4), lax.bitwise_xor(y, pair % 4)
                a, b = mine[from_y, from_zh, at], other[from_y, from_zh, at]
                tiles.append(jnp.where(core == j % 2, a, b))
            d_re = MU * jnp.swapaxes(jnp.stack(tiles), 0, 1) + shift_re
            step = lax.broadcasted_iota(jnp.int32, (ROWS, 8, 128), 0).astype(jnp.float32)
            row = start[...] + (step + first)
            inside = jnp.logical_and(row >= 0.0, row < 16.0 * ROWS)
            scale = jnp.where(inside, 1.0, 0.0) / (d_re * d_re + d_im * d_im)
            coef[first : first + ROWS, 0, j] = d_re * scale
            coef[first : first + ROWS, 1, j] = -d_im * scale


def swept(get, source, coef, row, c_row):
    lane = lax.broadcasted_iota(jnp.int32, (8, 128), 1)
    sublane = lax.broadcasted_iota(jnp.int32, (8, 128), 0)
    zero = jnp.zeros((8, 128), jnp.float32)

    def total(c):
        tiles = [get(row, c, j) for j in range(4)]
        below = [jnp.where(sublane == 0, zero, pltpu.roll(tiles[3], 1, 0))] + tiles[:3]
        above = tiles[1:] + [jnp.where(sublane == 7, zero, pltpu.roll(tiles[0], 7, 0))]
        sums = []
        for j in range(4):
            sides = jnp.where(lane == 0, zero, pltpu.roll(tiles[j], 1, 1))
            sides = sides + jnp.where(lane == 127, zero, pltpu.roll(tiles[j], 127, 1))
            outer = get(row - 1, c, j) + get(row + 1, c, j)
            sums.append(source(row, c, j) + MU * (((below[j] + above[j]) + outer) + sides))
        return sums

    return times_coefficient(coef, c_row, total(0), total(1))


def times_coefficient(coef, row, s_re, s_im):
    result = []
    for j in range(4):
        g_re, g_im = coef[row, 0, j], coef[row, 1, j]
        result.append((g_re * s_re[j] - g_im * s_im[j], g_re * s_im[j] + g_im * s_re[j]))
    return result


def put(ref, at, values):
    for j in range(4):
        ref[(*at, 0, j)] = values[j][0]
        ref[(*at, 1, j)] = values[j][1]


def first_fields(ref, rows, coef, c_first, write):
    def step(i, carry):
        s_re, s_im = ([ref[i, c, j] for j in range(4)] for c in range(2))
        write(i, times_coefficient(coef, c_first + i, s_re, s_im))
        return carry

    lax.fori_loop(0, rows, step, 0)


INNER = BLOCK // 2


def inner_kernel(own, coef, levels):
    first_fields(own, BLOCK, coef, HALO, lambda i, values: put(levels, (0, i), values))
    for m in range(1, INNER):
        for row in range(m, BLOCK - m):
            values = swept(
                lambda r, c, j, m=m: levels[m - 1, r, c, j],
                lambda r, c, j: own[r, c, j],
                coef,
                row,
                row + HALO,
            )
            put(levels, (m, row), values)


def sweep_kernel(link, die, own, coef, levels, out, u0, u1, left, right):
    fields = (u0, u1)
    behind = HALO + BLOCK
    odd = my_place() % 2

    def side(rows, first, from_die):
        def step(i, carry):
            s = [
                [jnp.where(odd == from_die, die[i, c, j], link[i, c, j]) for j in range(4)]
                for c in range(2)
            ]
            put(rows, (i,), list(zip(*s)))
            put(u0, (first + i,), times_coefficient(coef, first + i, *s))
            return carry

        lax.fori_loop(0, HALO, step, 0)

    side(left, 0, 1)
    side(right, behind, 0)

    def inside(m, row):
        return m < INNER and m <= row - HALO < BLOCK - m

    def source(row, c, j):
        if row < HALO:
            return left[row, c, j]
        return own[row - HALO, c, j] if row < behind else right[row - behind, c, j]

    def getter(m):
        def get(row, c, j):
            return levels[m, row - HALO, c, j] if inside(m, row) else fields[m % 2][row, c, j]

        return get

    for m in range(1, SWEEPS):
        for row in range(m, WINDOW - m):
            if inside(m, row):
                continue
            values = swept(getter(m - 1), source, coef, row, row)
            if m < SWEEPS - 1:
                put(fields[m % 2], (row,), values)
            else:
                put(out, (row - HALO,), values)


def call(kernel, shape, *args, scratch=()):
    return pl.pallas_call(
        kernel,
        out_shape=pltpu.VMEM(shape, jnp.float32),
        scratch_shapes=scratch,
        compiler_params=pltpu.CompilerParams(vmem_limit_bytes=VMEM),
    )(*[pltpu.with_memory_space_constraint(a, pltpu.VMEM) for a in args])


def near_reaction(reaction):
    near = jnp.pad(reaction, ((0, 0), (HALO, NEAR - 2 * BLOCK - HALO), (0, 0)))
    first = (lax.axis_index("core"), lax.axis_index("x") * 2 * BLOCK, 0)
    return lax.dynamic_slice(near, first, (1, NEAR, 128))[0]


def gathered(x, axis):
    others = [lax.ppermute(x, axis, [(i, i ^ d) for i in range(4)]) for d in (1, 2, 3)]
    return jnp.stack([x] + others)


def exchange(x, axes):
    return lax.all_to_all(x, axes, 0, 0, tiled=True)


def swaps(first):
    pairs = [
        (device_of(i, zl), device_of(i + 1, zl)) for zl in range(2) for i in range(first, 7, 2)
    ]
    return pairs + [(b, a) for a, b in pairs]


def stages(state_rhs, adjoint_rhs, reaction):
    sems = pltpu.SemaphoreType.DMA((32,))
    both = pl.pallas_call(
        pack_kernel,
        in_specs=[pl.BlockSpec(memory_space=pltpu.HBM)] * 2,
        out_shape=pltpu.VMEM((16, 2, 2, 2, ROWS, 128), jnp.float32),
        scratch_shapes=[sems],
        compiler_params=pltpu.CompilerParams(vmem_limit_bytes=VMEM),
        name="pack_kernel",
    )(*[pltpu.with_memory_space_constraint(a, pltpu.HBM) for a in (state_rhs, adjoint_rhs)])
    times = exchange(both, TIME)
    mine = gathered(gathered(near_reaction(reaction), "zh"), "y")
    other = lax.ppermute(mine, "core", [(0, 1), (1, 0)])
    shifts = [call(kernel, (8, 128)) for kernel in (real_kernel, imaginary_kernel, start_kernel)]
    coef = call(coefficient_kernel, (PADDED, 2, 4, 8, 128), mine, other, *shifts)
    hat = call(forward_kernel, (STEPS, 2, 2, ROWS, 128), times)
    got = exchange(hat, FREQ)
    got = got.reshape(2, 2, 2, 4, 2, 2, ROWS, 128)
    own = call(planes_to_rows_kernel, (BLOCK, 2, 4, 8, 128), got)
    odd = my_place() % 2
    last = odd * (BLOCK - HALO)
    link = lax.ppermute(lax.dynamic_slice_in_dim(own, last, HALO), TM, swaps(1))
    other_side = lax.dynamic_slice_in_dim(own, BLOCK - HALO - last, HALO)
    die = lax.ppermute(other_side, TM, swaps(0))
    levels = call(inner_kernel, (INNER, BLOCK, 2, 4, 8, 128), own, coef)
    window = pltpu.VMEM((WINDOW, 2, 4, 8, 128), jnp.float32)
    block = (BLOCK, 2, 4, 8, 128)
    edge = pltpu.VMEM((HALO, 2, 4, 8, 128), jnp.float32)
    scratch = [window] * 2 + [edge] * 2
    solved = call(sweep_kernel, block, link, die, own, coef, levels, scratch=scratch)
    solved = call(rows_to_planes_kernel, (2, 2, 2, 4, 2, 2, ROWS, 128), solved)
    by_freq = exchange(solved.reshape(STEPS, 2, 2, ROWS, 128), FREQ)
    by_time = call(backward_kernel, (16, 2, 2, 2, ROWS, 128), by_freq)
    final = exchange(by_time, TIME)
    return pl.pallas_call(
        unpack_kernel,
        out_specs=[pl.BlockSpec(memory_space=pltpu.HBM)] * 2,
        out_shape=[jax.ShapeDtypeStruct(state_rhs.shape, jnp.float32)] * 2,
        scratch_shapes=[sems],
        compiler_params=pltpu.CompilerParams(vmem_limit_bytes=VMEM),
        name="unpack_kernel",
    )(pltpu.with_memory_space_constraint(final, pltpu.VMEM))


def solution(mesh):
    split = Mesh(mesh.devices.reshape(4, 2, 2, 4, 4), TM + SPACE)
    field = P(TM, SPACE, None, None)
    return jax.shard_map(
        stages,
        mesh=split,
        in_specs=(field, field, P(SPACE, None, None)),
        out_specs=(field, field),
        check_vma=False,
    )
```
